256 devices in a mesh: act: 64 (over x, z, core), rep: 4 (over y).
Axes of the slice: x: 4, y: 4, z: 8, core: 2. Of those that a mesh axis runs over, the one named last changes fastest.
Arguments:
- estimated_returns: float32 [512, 131072], P('act', 'rep'), may hold values from -1000 to 1000
- chosen_move_ids: int32 [512, 131072], P('act', 'rep'), may hold values from 0 to 17
- previous_eta: float32 [1], replicated, may hold values from 0.3 to 3
- trust_region_epsilon: float32 [1], replicated, may hold values from 0.02 to 1
Outputs:
- sample_importance: float32 [512, 131072], P('act', 'rep')
- goal_distribution: float32 [18, 131072], P(None, ('rep', 'act'))
- new_temperature: float32 [1], replicated
The draws below stay inside these ranges and needn't reach their ends.
All inputs are finite; a program needn't handle non-finite values.
Results may differ from the reference program's by a relative error of at most 0.0003.
Values sent between devices are 32-bit elements; how exact they have to be, the bound alone decides.
No kernel may reach another device: no remote copies, remote signals or barrier semaphores. Data moves between devices by JAX's collectives and lax.ppermute only.
A program may use at most 64 MiB of HBM per device.

```python
import math
import jax
import jax.numpy as jnp

SAMPLE_COUNT = 512
NACT = 18
ITERS = 3
STATE_DEV = 512
STATES = 131072


def draw_estimated_returns(key, part):
    key_base = jax.random.fold_in(key, 11)
    key_scale = jax.random.fold_in(key, 12)
    key_block = jax.random.fold_in(key, 13)
    key_shift = jax.random.fold_in(key, 14)
    base = jax.random.truncated_normal(key_base, -4.0, 4.0, (SAMPLE_COUNT, STATES), jnp.float32)
    scale_per_row = jnp.exp(jax.random.uniform(key_scale, (STATES,), jnp.float32, jnp.log(0.3), jnp.log(3.0)))
    block_scale = jnp.exp(jax.random.uniform(key_block, (STATES // STATE_DEV,), jnp.float32, jnp.log(0.5), jnp.log(2.0)))
    block_scale = jnp.repeat(block_scale, STATE_DEV)
    offset = jax.random.uniform(key_shift, (STATES,), jnp.float32, -5.0, 5.0)
    return base * (scale_per_row * block_scale)[None, :] + offset[None, :]


def touch_ends(result, rng, smallest, top_value):
    shape = result.shape
    spot = [jax.random.randint(jax.random.fold_in(rng, axis), (), 0, shape[axis]) for axis in range(len(shape))]
    result = result.at[tuple(spot)].set(smallest)
    longest = shape.index(max(shape))
    spot[longest] = (spot[longest] + 1) % shape[longest]
    return result.at[tuple(spot)].set(top_value)


def setup_inputs(seed: int = 0) -> dict:
    arg_keys = jax.random.split(jax.random.key(seed), 5)
    return {
        "estimated_returns": draw_estimated_returns(jax.random.fold_in(arg_keys[4], 71), 0),
        "chosen_move_ids": touch_ends(jax.random.randint(arg_keys[1], (SAMPLE_COUNT, STATES), 0, NACT), jax.random.fold_in(arg_keys[1], 1), 0, NACT - 1).astype(jnp.int32),
        "previous_eta": jnp.clip(jnp.exp(jax.random.uniform(arg_keys[2], (1,), jnp.float32, math.log(0.3), math.log(3.0))), 0.3, 3.0),
        "trust_region_epsilon": jnp.clip(jnp.exp(jax.random.uniform(arg_keys[3], (1,), jnp.float32, math.log(0.02), math.log(1.0))), 0.02, 1.0),
    }


def summary_figures(centered_returns, lagrange_eta):
    exponential_term = jnp.exp(centered_returns / lagrange_eta)
    partition_total = jnp.sum(exponential_term, axis=0)
    leading_part = jnp.sum(exponential_term * centered_returns, axis=0)
    trailing_part = jnp.sum(exponential_term * centered_returns * centered_returns, axis=0)
    return exponential_term, partition_total, leading_part, trailing_part


def reference(estimated_returns, chosen_move_ids, previous_eta, trust_region_epsilon):
    lagrange_eta = previous_eta[0]
    ceiling_term = trust_region_epsilon[0]
    centered_returns = estimated_returns - jnp.max(estimated_returns, axis=0, keepdims=True)
    for step in range(ITERS):
        exponential_term, partition_total, leading_part, trailing_part = summary_figures(centered_returns, lagrange_eta)
        entropy_gap = leading_part / (partition_total * lagrange_eta) - jnp.log(partition_total) + jnp.log(jnp.float32(SAMPLE_COUNT))
        mean_first = leading_part / partition_total
        spread = trailing_part / partition_total - mean_first * mean_first
        aggregate_relative_entropy = jnp.sum(entropy_gap) / STATES
        aggregate_deviation = jnp.sum(spread) / STATES
        change_amount = (ceiling_term - aggregate_relative_entropy) * lagrange_eta / (1.0 + aggregate_deviation / lagrange_eta)
        lagrange_eta = lagrange_eta * jnp.exp(-jnp.tanh(change_amount))
    exponential_term, partition_total, leading_part, trailing_part = summary_figures(centered_returns, lagrange_eta)
    probs = exponential_term / partition_total
    sample_importance = SAMPLE_COUNT * probs
    goal_distribution = jnp.stack([jnp.sum(jnp.where(chosen_move_ids == k, probs, 0.0), axis=0) for k in range(NACT)])
    return sample_importance, goal_distribution, jnp.reshape(lagrange_eta, (1,))
```

```python
import functools
import jax
import jax.numpy as jnp
from jax import lax
from jax.experimental import pallas as pl
from jax.experimental.pallas import tpu as pltpu
from jax.sharding import PartitionSpec as P

NACT = 18
ITERS = 3
LANES = 128
ALL = ("rep", "act")
VMEM = pl.BlockSpec(memory_space=pltpu.VMEM)
SMEM = pl.BlockSpec(memory_space=pltpu.SMEM)
PARAMS = pltpu.CompilerParams(vmem_limit_bytes=8 * 1024 * 1024)


def call(body, out_shape, name, n_smem, n_vmem, flops=1_000_000):
    n_out = len(out_shape) if isinstance(out_shape, (tuple, list)) else None
    return pl.pallas_call(
        body,
        out_shape=out_shape,
        in_specs=[SMEM] * n_smem + [VMEM] * n_vmem,
        out_specs=VMEM if n_out is None else [VMEM] * n_out,
        compiler_params=PARAMS,
        cost_estimate=pl.CostEstimate(flops=flops, bytes_accessed=2_000_000, transcendentals=262_144),
        name=name,
    )


def partial_sums(q_ref, top, eta, samples):
    blocks, rows, states = q_ref.shape
    inverse = jnp.broadcast_to((1.0 / eta)[:, :1], (rows, states))
    top_rows = jnp.broadcast_to(top, (rows, states))

    def step(i, sums):
        z, c1, c2 = sums
        shifted = q_ref[i] - top_rows
        expo = jnp.exp(shifted * inverse)
        first = expo * shifted
        return z + expo, c1 + first, c2 + first * shifted

    zero = jnp.zeros((rows, states), jnp.float32)
    z, c1, c2 = lax.fori_loop(0, blocks, step, (zero, zero, zero), unroll=8)
    z, c1, c2 = (jnp.sum(v, axis=0, keepdims=True) for v in (z, c1, c2))
    mean = c1 / z
    kl = mean * inverse[:1] - jnp.log(z) + jnp.log(jnp.float32(samples))
    spread = c2 / z - mean * mean
    lane = lax.broadcasted_iota(jnp.int32, (1, LANES), 1)
    kl_sum = jnp.sum(kl, axis=1, keepdims=True)
    spread_sum = jnp.sum(spread, axis=1, keepdims=True)
    return jnp.where(lane == 0, kl_sum, jnp.where(lane == 1, spread_sum, 0.0))


def next_eta(gathered_ref, eta, eps, states):
    total = jnp.sum(gathered_ref[...], axis=0) * jnp.float32(1.0 / states)
    divergence = jnp.broadcast_to(total[:, 0:1], eta.shape)
    deviation = jnp.broadcast_to(total[:, 1:2], eta.shape)
    change = (eps - divergence) * eta / (1.0 + deviation / eta)
    return eta * jnp.exp(-jnp.tanh(change))


def row(scalar):
    return jnp.full((1, LANES), scalar, jnp.float32)


def first_body(samples, eta_ref, q_ref, top_ref, eta_out, part_ref):
    top8 = q_ref[0]
    top8 = lax.fori_loop(1, q_ref.shape[0], lambda i, m: jnp.maximum(m, q_ref[i]), top8)
    top = jnp.max(top8, axis=0, keepdims=True)
    top_ref[...] = top
    eta = row(eta_ref[0])
    eta_out[...] = eta
    part_ref[...] = jnp.broadcast_to(partial_sums(q_ref, top, eta, samples)[None], part_ref.shape)


def step_body(samples, states, eps_ref, q_ref, top_ref, eta_ref, gathered_ref, eta_out, part_ref):
    eta = next_eta(gathered_ref, eta_ref[...], row(eps_ref[0]), states)
    eta_out[...] = eta
    part_ref[...] = jnp.broadcast_to(partial_sums(q_ref, top_ref[...], eta, samples)[None], part_ref.shape)


def last_body(samples, states, eps_ref, q_ref, top_ref, eta_ref, gathered_ref, eta_out, back_ref):
    eta = next_eta(gathered_ref, eta_ref[...], row(eps_ref[0]), states)
    eta_out[...] = eta
    blocks, rows, width = q_ref.shape
    inverse = jnp.broadcast_to((1.0 / eta)[:, :1], (rows, width))
    top = top_ref[...]
    top_rows = jnp.broadcast_to(top, (rows, width))
    z = lax.fori_loop(
        0, blocks, lambda i, z: z + jnp.exp((q_ref[i] - top_rows) * inverse),
        jnp.zeros((rows, width), jnp.float32), unroll=8)
    scale = jnp.float32(samples) / jnp.sum(z, axis=0, keepdims=True)
    copies = back_ref.shape[0]
    back_ref[:, :, :width] = jnp.broadcast_to(top[None], (copies, 1, width))
    back_ref[:, :, width:] = jnp.broadcast_to(scale[None], (copies, 1, width))


def goal_body(samples, q_ref, ids_ref, back_ref, eta_ref, goal_ref):
    blocks, rows, width = q_ref.shape
    inverse = jnp.broadcast_to((1.0 / eta_ref[...])[:, :1], (rows, LANES))
    for tile in range(width // LANES):
        at = slice(tile * LANES, (tile + 1) * LANES)
        top_rows = jnp.broadcast_to(back_ref[0, :, at], (rows, LANES))
        scale = back_ref[0, :, width + tile * LANES : width + (tile + 1) * LANES] * jnp.float32(1.0 / samples)

        def step(i, sums):
            expo = jnp.exp((q_ref[i, :, at] - top_rows) * inverse)
            ids = ids_ref[i, :, at]
            return tuple(s + jnp.where(ids == k, expo, 0.0) for k, s in enumerate(sums))

        zero = jnp.zeros((rows, LANES), jnp.float32)
        sums = lax.fori_loop(0, blocks, step, (zero,) * NACT, unroll=2)
        for k, s in enumerate(sums):
            goal_ref[k : k + 1, at] = jnp.sum(s, axis=0, keepdims=True) * scale


def weights_body(eta_ref, x_ref, back_ref, out_ref):
    rows, width = x_ref.shape
    owners, _, both = back_ref.shape
    own = both // 2
    inverse = jnp.broadcast_to((1.0 / eta_ref[...])[:, :1], (rows, own))
    for j in range(owners):
        at = slice(j * own, (j + 1) * own)
        top = jnp.broadcast_to(back_ref[j, :, :own], (rows, own))
        scale = jnp.broadcast_to(back_ref[j, :, own:], (rows, own))
        out_ref[:, at] = jnp.exp((x_ref[:, at] - top) * inverse) * scale


def send(blocks, axis):
    return lax.all_to_all(blocks, axis, split_axis=0, concat_axis=0, tiled=True)


def on_device(estimated_returns, chosen_move_ids, previous_eta, trust_region_epsilon):
    peers = lax.axis_size("act")
    everyone = peers * lax.axis_size("rep")
    rows, width = estimated_returns.shape
    own = width // peers
    samples, states = rows * peers, width * lax.axis_size("rep")
    f32 = jnp.float32
    shape = jax.ShapeDtypeStruct

    def to_owner(v):
        return send(v.reshape(rows, peers, own).transpose(1, 0, 2), "act")

    q = to_owner(estimated_returns)
    ids = to_owner(chosen_move_ids)

    eta_shape, part_shape = shape((1, LANES), f32), shape((everyone, 1, LANES), f32)
    top, eta, part = call(
        functools.partial(first_body, samples), [shape((1, own), f32), eta_shape, part_shape], "first", 1, 1
    )(previous_eta, q)
    for _ in range(ITERS - 1):
        gathered = send(part, ALL)
        eta, part = call(
            functools.partial(step_body, samples, states), [eta_shape, part_shape], "step", 1, 4
        )(trust_region_epsilon, q, top, eta, gathered)
    gathered = send(part, ALL)
    eta, back = call(
        functools.partial(last_body, samples, states),
        [eta_shape, shape((peers, 1, 2 * own), f32)], "last", 1, 4,
    )(trust_region_epsilon, q, top, eta, gathered)
    everywhere = send(back, "act")
    goal = call(
        functools.partial(goal_body, samples), shape((NACT, own), f32), "goal", 0, 4, flops=20_000_000
    )(q, ids, back, eta)

    steps = 8
    weights = pl.pallas_call(
        weights_body,
        grid=(steps,),
        out_shape=shape((rows, width), f32),
        in_specs=[
            pl.BlockSpec((1, LANES), lambda i: (0, 0)),
            pl.BlockSpec((rows, width // steps), lambda i: (0, i)),
            pl.BlockSpec((peers // steps, 1, 2 * own), lambda i: (i, 0, 0)),
        ],
        out_specs=pl.BlockSpec((rows, width // steps), lambda i: (0, i)),
        compiler_params=PARAMS,
        cost_estimate=pl.CostEstimate(flops=1_000_000, bytes_accessed=2_000_000, transcendentals=262_144),
        name="weights",
    )(eta, estimated_returns, everywhere)
    return weights, goal, eta[0, :1]


def solution(mesh):
    placed = (P("act", "rep"), P("act", "rep"), P(), P())
    return jax.shard_map(
        on_device,
        mesh=mesh,
        in_specs=placed,
        out_specs=(P("act", "rep"), P(None, ALL), P()),
        check_vma=False,
    )
```

```python
import functools
import jax
import jax.numpy as jnp
from jax import lax
from jax.experimental import pallas as pl
from jax.experimental.pallas import tpu as pltpu
from jax.sharding import Mesh
from jax.sharding import PartitionSpec as P

NACT = 18
ITERS = 3
LANES = 128
ACT = ("x", "z", "core")
ALL = ("rep", "x", "z", "core")
VMEM = pl.BlockSpec(memory_space=pltpu.VMEM)
SMEM = pl.BlockSpec(memory_space=pltpu.SMEM)
PARAMS = pltpu.CompilerParams(vmem_limit_bytes=8 * 1024 * 1024)


def call(body, out_shape, n_smem, n_vmem, flops=1_000_000):
    n_out = len(out_shape) if isinstance(out_shape, (tuple, list)) else None
    return pl.pallas_call(
        body,
        out_shape=out_shape,
        in_specs=[SMEM] * n_smem + [VMEM] * n_vmem,
        out_specs=VMEM if n_out is None else [VMEM] * n_out,
        compiler_params=PARAMS,
        cost_estimate=pl.CostEstimate(flops=flops, bytes_accessed=2_000_000, transcendentals=262_144),
    )


def partial_sums(q_ref, top, eta, samples):
    blocks, rows, states = q_ref.shape
    inverse = jnp.broadcast_to((1.0 / eta)[:, :1], (rows, states))
    top_rows = jnp.broadcast_to(top, (rows, states))

    def step(i, sums):
        z, c1, c2 = sums
        shifted = q_ref[i] - top_rows
        expo = jnp.exp(shifted * inverse)
        first = expo * shifted
        return z + expo, c1 + first, c2 + first * shifted

    zero = jnp.zeros((rows, states), jnp.float32)
    z, c1, c2 = lax.fori_loop(0, blocks, step, (zero, zero, zero), unroll=8)
    z, c1, c2 = (jnp.sum(v, axis=0, keepdims=True) for v in (z, c1, c2))
    mean = c1 / z
    kl = mean * inverse[:1] - jnp.log(z) + jnp.log(jnp.float32(samples))
    spread = c2 / z - mean * mean
    lane = lax.broadcasted_iota(jnp.int32, (1, LANES), 1)
    kl_sum = jnp.sum(kl, axis=1, keepdims=True)
    spread_sum = jnp.sum(spread, axis=1, keepdims=True)
    return jnp.where(lane == 0, kl_sum, jnp.where(lane == 1, spread_sum, 0.0))


def next_eta(gathered_ref, eta, eps, states):
    total = jnp.sum(gathered_ref[...], axis=0) * jnp.float32(1.0 / states)
    divergence = jnp.broadcast_to(total[:, 0:1], eta.shape)
    deviation = jnp.broadcast_to(total[:, 1:2], eta.shape)
    change = (eps - divergence) * eta / (1.0 + deviation / eta)
    return eta * jnp.exp(-jnp.tanh(change))


def row(scalar):
    return jnp.full((1, LANES), scalar, jnp.float32)


def first_body(samples, eta_ref, eps_ref, q_ref, top_ref, eta_out, eps_out, part_ref):
    top8 = q_ref[0]
    top8 = lax.fori_loop(1, q_ref.shape[0], lambda i, m: jnp.maximum(m, q_ref[i]), top8)
    top = jnp.max(top8, axis=0, keepdims=True)
    top_ref[...] = top
    eta = row(eta_ref[0])
    eta_out[...] = eta
    eps_out[...] = row(eps_ref[0])
    part_ref[...] = jnp.broadcast_to(partial_sums(q_ref, top, eta, samples)[None], part_ref.shape)


def step_body(samples, states, eps_ref, q_ref, top_ref, eta_ref, gathered_ref, eta_out, part_ref):
    eta = next_eta(gathered_ref, eta_ref[...], eps_ref[...], states)
    eta_out[...] = eta
    part_ref[...] = jnp.broadcast_to(partial_sums(q_ref, top_ref[...], eta, samples)[None], part_ref.shape)


def last_body(samples, states, eps_ref, q_ref, top_ref, eta_ref, gathered_ref, eta_out, back_ref):
    eta = next_eta(gathered_ref, eta_ref[...], eps_ref[...], states)
    eta_out[...] = eta
    blocks, rows, width = q_ref.shape
    inverse = jnp.broadcast_to((1.0 / eta)[:, :1], (rows, width))
    top = top_ref[...]
    top_rows = jnp.broadcast_to(top, (rows, width))
    z = lax.fori_loop(
        0, blocks, lambda i, z: z + jnp.exp((q_ref[i] - top_rows) * inverse),
        jnp.zeros((rows, width), jnp.float32), unroll=8)
    scale = jnp.float32(samples) / jnp.sum(z, axis=0, keepdims=True)
    copies = back_ref.shape[0]
    back_ref[:, :, :width] = jnp.broadcast_to(top[None], (copies, 1, width))
    back_ref[:, :, width:] = jnp.broadcast_to(scale[None], (copies, 1, width))


def split_body(at_ref, ids_ref, from_core_ref, *out_refs):
    z, core = at_ref[1], at_ref[2]
    hops = len(out_refs)
    for k, out_ref in enumerate(out_refs):
        to = lax.rem(z + k, hops)
        for x in range(out_ref.shape[1]):
            out_ref[0, x] = ids_ref[x, to, core]
            out_ref[1, x] = from_core_ref[x, to]


def merge_body(at_ref, _, *refs):
    hops = len(refs) * 2 // 3
    in_refs, out_refs = refs[:hops], refs[hops:]
    for j, out_ref in enumerate(out_refs):
        to = lax.rem(at_ref[0] + j, len(out_refs))
        for k, in_ref in enumerate(in_refs):
            out_ref[k] = in_ref[:, to]


def goal_body(samples, at_ref, q_ref, back_ref, eta_ref, *refs):
    ids_refs, goal_ref = refs[:-1], refs[-1]
    across, along, cores = len(ids_refs), ids_refs[0].shape[0], ids_refs[0].shape[1]
    _, rows, width = q_ref.shape
    inverse = jnp.broadcast_to((1.0 / eta_ref[...])[:, :1], (rows, LANES))
    x, z, core = at_ref[0], at_ref[1], at_ref[2]
    for tile in range(width // LANES):
        at = slice(tile * LANES, (tile + 1) * LANES)
        top_rows = jnp.broadcast_to(back_ref[0, :, at], (rows, LANES))
        scale = back_ref[0, :, width + tile * LANES : width + (tile + 1) * LANES] * jnp.float32(1.0 / samples)
        sums = (jnp.zeros((rows, LANES), jnp.float32),) * NACT
        for j, ids_ref in enumerate(ids_refs):
            from_x = lax.rem(x + across - j, across)

            def step(k, sums):
                from_z = lax.rem(z + along - k, along)
                for c in range(cores):
                    from_core = core if c == 0 else 1 - core
                    holder = (from_x * along + from_z) * cores + from_core
                    expo = jnp.exp((q_ref[holder, :, at] - top_rows) * inverse)
                    ids = ids_ref[k, c, :, at]
                    sums = tuple(s + jnp.where(ids == n, expo, 0.0) for n, s in enumerate(sums))
                return sums

            sums = lax.fori_loop(0, along, step, sums)
        for n, s in enumerate(sums):
            goal_ref[n : n + 1, at] = jnp.sum(s, axis=0, keepdims=True) * scale


def weights_body(eta_ref, x_ref, back_ref, out_ref):
    rows, _ = x_ref.shape
    owners, _, both = back_ref.shape
    own = both // 2
    inverse = jnp.broadcast_to((1.0 / eta_ref[...])[:, :1], (rows, own))
    for j in range(owners):
        at = slice(j * own, (j + 1) * own)
        top = jnp.broadcast_to(back_ref[j, :, :own], (rows, own))
        scale = jnp.broadcast_to(back_ref[j, :, own:], (rows, own))
        out_ref[:, at] = jnp.exp((x_ref[:, at] - top) * inverse) * scale


def send(blocks, axis):
    return lax.all_to_all(blocks, axis, split_axis=0, concat_axis=0, tiled=True)


def shifted_by(v, axis, hops):
    size = lax.axis_size(axis)
    return lax.ppermute(v, axis, [(i, (i + hops) % size) for i in range(size)])


def on_device(estimated_returns, chosen_move_ids, previous_eta, trust_region_epsilon):
    across, along, cores = (lax.axis_size(a) for a in ACT)
    peers = lax.axis_size(ACT)
    everyone = peers * lax.axis_size("rep")
    rows, width = estimated_returns.shape
    own = width // peers
    samples, states = rows * peers, width * lax.axis_size("rep")
    f32, i32 = jnp.float32, jnp.int32
    shape = jax.ShapeDtypeStruct
    at = jnp.stack([lax.axis_index(a) for a in ACT])

    def by_owner(v):
        return v.reshape(rows, peers, own).transpose(1, 0, 2)

    q = send(by_owner(estimated_returns), ACT)

    moves = by_owner(chosen_move_ids).reshape(across, along, cores, rows, own)
    give = lax.dynamic_index_in_dim(moves, 1 - at[2], 2, keepdims=False)
    from_core = shifted_by(give, "core", 1)
    chunks = call(split_body, [shape((cores, across, rows, own), i32)] * along, 1, 2)(at, moves, from_core)
    arrived = [chunks[0]]
    for k in range(1, along):
        arrived.append(shifted_by(chunks[k], "z", k))

    row_shape, part_shape = shape((1, LANES), f32), shape((everyone, 1, LANES), f32)
    top, eta, eps, part = call(
        functools.partial(first_body, samples), [shape((1, own), f32), row_shape, row_shape, part_shape], 2, 1
    )(previous_eta, trust_region_epsilon, q)
    for i in range(ITERS - 1):
        gathered = send(part, ALL)
        eta, part = call(
            functools.partial(step_body, samples, states), [row_shape, part_shape], 0, 5
        )(eps, q, top, eta, gathered)
        if i == 1:
            chunks = call(merge_body, [shape((along, cores, rows, own), i32)] * across, 1, 1 + along)(at, eta, *arrived)
            ids = [chunks[0]]
            for j in range(1, across):
                ids.append(shifted_by(chunks[j], "x", j))
    gathered = send(part, ALL)
    eta, back = call(
        functools.partial(last_body, samples, states),
        [row_shape, shape((peers, 1, 2 * own), f32)], 0, 5,
    )(eps, q, top, eta, gathered)
    everywhere = send(back, ACT)
    goal = call(
        functools.partial(goal_body, samples), shape((NACT, own), f32), 1, 3 + across, flops=20_000_000
    )(at, q, back, eta, *ids)

    steps = 8
    weights = pl.pallas_call(
        weights_body,
        grid=(steps,),
        out_shape=shape((rows, width), f32),
        in_specs=[
            pl.BlockSpec((1, LANES), lambda i: (0, 0)),
            pl.BlockSpec((rows, width // steps), lambda i: (0, i)),
            pl.BlockSpec((peers // steps, 1, 2 * own), lambda i: (i, 0, 0)),
        ],
        out_specs=pl.BlockSpec((rows, width // steps), lambda i: (0, i)),
        compiler_params=PARAMS,
        cost_estimate=pl.CostEstimate(flops=1_000_000, bytes_accessed=2_000_000, transcendentals=262_144),
        name="weights",
    )(eta, estimated_returns, everywhere)
    return weights, goal, eta[0, :1]


def solution(mesh):
    split = Mesh(mesh.devices.reshape(4, 8, 2, mesh.shape["rep"]), (*ACT, "rep"))
    placed = (P(ACT, "rep"), P(ACT, "rep"), P(), P())
    return jax.shard_map(
        on_device,
        mesh=split,
        in_specs=placed,
        out_specs=(P(ACT, "rep"), P(None, ALL), P()),
        check_vma=False,
    )
```

```python
import functools
import jax
import jax.numpy as jnp
from jax import lax
from jax.experimental import pallas as pl
from jax.experimental.pallas import tpu as pltpu
from jax.sharding import Mesh
from jax.sharding import PartitionSpec as P

NACT = 18
ITERS = 3
LANES = 128
ACT = ("x", "z", "core")
ALL = ("rep", "x", "z", "core")
CHIPS = ("rep", "x", "z")
PLANE = ("x", "z")
VMEM = pl.BlockSpec(memory_space=pltpu.VMEM)
SMEM = pl.BlockSpec(memory_space=pltpu.SMEM)
PARAMS = pltpu.CompilerParams(vmem_limit_bytes=8 * 1024 * 1024)


def call(body, out_shape, n_smem, n_vmem, flops=1_000_000):
    n_out = len(out_shape) if isinstance(out_shape, (tuple, list)) else None
    return pl.pallas_call(
        body,
        out_shape=out_shape,
        in_specs=[SMEM] * n_smem + [VMEM] * n_vmem,
        out_specs=VMEM if n_out is None else [VMEM] * n_out,
        compiler_params=PARAMS,
        cost_estimate=pl.CostEstimate(flops=flops, bytes_accessed=2_000_000, transcendentals=262_144),
    )


def partial_sums(q_ref, top, eta, samples):
    blocks, rows, states = q_ref.shape
    inverse = jnp.broadcast_to((1.0 / eta)[:, :1], (rows, states))
    top_rows = jnp.broadcast_to(top, (rows, states))

    def step(i, sums):
        z, c1, c2 = sums
        shifted = q_ref[i] - top_rows
        expo = jnp.exp(shifted * inverse)
        first = expo * shifted
        return z + expo, c1 + first, c2 + first * shifted

    zero = jnp.zeros((rows, states), jnp.float32)
    z, c1, c2 = lax.fori_loop(0, blocks, step, (zero, zero, zero), unroll=8)
    z, c1, c2 = (jnp.sum(v, axis=0, keepdims=True) for v in (z, c1, c2))
    mean = c1 / z
    kl = mean * inverse[:1] - jnp.log(z) + jnp.log(jnp.float32(samples))
    spread = c2 / z - mean * mean
    lane = lax.broadcasted_iota(jnp.int32, (1, LANES), 1)
    kl_sum = jnp.sum(kl, axis=1, keepdims=True)
    spread_sum = jnp.sum(spread, axis=1, keepdims=True)
    return jnp.where(lane == 0, kl_sum, jnp.where(lane == 1, spread_sum, 0.0))


def next_eta(gathered_ref, eta, eps, states):
    total = jnp.sum(gathered_ref[...], axis=0) * jnp.float32(1.0 / states)
    divergence = jnp.broadcast_to(total[:, 0:1], eta.shape)
    deviation = jnp.broadcast_to(total[:, 1:2], eta.shape)
    change = (eps - divergence) * eta / (1.0 + deviation / eta)
    return eta * jnp.exp(-jnp.tanh(change))


def row(scalar):
    return jnp.full((1, LANES), scalar, jnp.float32)


def first_body(samples, eta_ref, eps_ref, q_ref, top_ref, eta_out, eps_out, part_ref):
    top8 = q_ref[0]
    top8 = lax.fori_loop(1, q_ref.shape[0], lambda i, m: jnp.maximum(m, q_ref[i]), top8)
    top = jnp.max(top8, axis=0, keepdims=True)
    top_ref[...] = top
    eta = row(eta_ref[0])
    eta_out[...] = eta
    eps_out[...] = row(eps_ref[0])
    part_ref[...] = partial_sums(q_ref, top, eta, samples)


def step_body(samples, states, eps_ref, q_ref, top_ref, eta_ref, gathered_ref, eta_out, part_ref):
    eta = next_eta(gathered_ref, eta_ref[...], eps_ref[...], states)
    eta_out[...] = eta
    part_ref[...] = partial_sums(q_ref, top_ref[...], eta, samples)


def last_body(samples, states, eps_ref, q_ref, top_ref, eta_ref, gathered_ref, eta_out, back_ref):
    eta = next_eta(gathered_ref, eta_ref[...], eps_ref[...], states)
    eta_out[...] = eta
    blocks, rows, width = q_ref.shape
    inverse = jnp.broadcast_to((1.0 / eta)[:, :1], (rows, width))
    top = top_ref[...]
    top_rows = jnp.broadcast_to(top, (rows, width))
    z = lax.fori_loop(
        0, blocks, lambda i, z: z + jnp.exp((q_ref[i] - top_rows) * inverse),
        jnp.zeros((rows, width), jnp.float32), unroll=8)
    scale = jnp.float32(samples) / jnp.sum(z, axis=0, keepdims=True)
    copies = back_ref.shape[0]
    back_ref[:, :, :width] = jnp.broadcast_to(top[None], (copies, 1, width))
    back_ref[:, :, width:] = jnp.broadcast_to(scale[None], (copies, 1, width))


def split_body(at_ref, ids_ref, from_core_ref, *out_refs):
    z, core = at_ref[1], at_ref[2]
    hops = len(out_refs)
    for k, out_ref in enumerate(out_refs):
        to = lax.rem(z + k, hops)
        for x in range(out_ref.shape[1]):
            out_ref[0, x] = ids_ref[x, to, core]
            out_ref[1, x] = from_core_ref[x, to]


def merge_body(at_ref, _, *refs):
    hops = len(refs) * 2 // 3
    in_refs, out_refs = refs[:hops], refs[hops:]
    for j, out_ref in enumerate(out_refs):
        to = lax.rem(at_ref[0] + j, len(out_refs))
        for k, in_ref in enumerate(in_refs):
            out_ref[k] = in_ref[:, to]


def goal_body(samples, at_ref, q_ref, back_ref, eta_ref, *refs):
    ids_refs, goal_ref = refs[:-1], refs[-1]
    across, along, cores = len(ids_refs), ids_refs[0].shape[0], ids_refs[0].shape[1]
    _, rows, width = q_ref.shape
    inverse = jnp.broadcast_to((1.0 / eta_ref[...])[:, :1], (rows, LANES))
    x, z, core = at_ref[0], at_ref[1], at_ref[2]
    for tile in range(width // LANES):
        at = slice(tile * LANES, (tile + 1) * LANES)
        top_rows = jnp.broadcast_to(back_ref[0, :, at], (rows, LANES))
        scale = back_ref[0, :, width + tile * LANES : width + (tile + 1) * LANES] * jnp.float32(1.0 / samples)
        sums = (jnp.zeros((rows, LANES), jnp.float32),) * NACT
        for j, ids_ref in enumerate(ids_refs):
            from_x = lax.rem(x + across - j, across)

            def step(k, sums):
                from_z = lax.rem(z + along - k, along)
                for c in range(cores):
                    from_core = core if c == 0 else 1 - core
                    holder = (from_x * along + from_z) * cores + from_core
                    expo = jnp.exp((q_ref[holder, :, at] - top_rows) * inverse)
                    ids = ids_ref[k, c, :, at]
                    sums = tuple(s + jnp.where(ids == n, expo, 0.0) for n, s in enumerate(sums))
                return sums

            sums = lax.fori_loop(0, along, step, sums)
        for n, s in enumerate(sums):
            goal_ref[n : n + 1, at] = jnp.sum(s, axis=0, keepdims=True) * scale


def weights_body(steps, at_ref, eta_ref, x_ref, same_ref, other_ref, out_ref, held, sems):
    rows, width = x_ref.shape
    chips, _, both = same_ref.shape
    own = both // 2
    inverse = jnp.broadcast_to((1.0 / eta_ref[...])[:, :1], (rows, own))
    core = at_ref[2]
    copies = []
    for step in range(steps):
        for chip in range(step * chips // steps, (step + 1) * chips // steps):
            for from_ref, owner in ((same_ref, chip * 2 + core), (other_ref, chip * 2 + 1 - core)):
                at = pl.ds(pl.multiple_of(owner * own, own), own)
                top = jnp.broadcast_to(from_ref[chip, :, :own], (rows, own))
                scale = jnp.broadcast_to(from_ref[chip, :, own:], (rows, own))
                held[:, at] = jnp.exp((x_ref[:, at] - top) * inverse) * scale
        part = pl.ds(step * width // steps, width // steps)
        copies.append(pltpu.make_async_copy(held.at[:, part], out_ref.at[:, part], sems.at[step]))
        copies[-1].start()
    for copy in copies:
        copy.wait()


def send(blocks, axis):
    return lax.all_to_all(blocks, axis, split_axis=0, concat_axis=0, tiled=True)


def shifted_by(v, axis, hops):
    size = lax.axis_size(axis)
    return lax.ppermute(v, axis, [(i, (i + hops) % size) for i in range(size)])


def on_device(estimated_returns, chosen_move_ids, previous_eta, trust_region_epsilon):
    across, along, cores = (lax.axis_size(a) for a in ACT)
    peers = lax.axis_size(ACT)
    everyone = peers * lax.axis_size("rep")
    rows, width = estimated_returns.shape
    own = width // peers
    samples, states = rows * peers, width * lax.axis_size("rep")
    f32, i32 = jnp.float32, jnp.int32
    shape = jax.ShapeDtypeStruct
    at = jnp.stack([lax.axis_index(a) for a in ACT])

    def by_owner(v):
        return v.reshape(rows, peers, own).transpose(1, 0, 2)

    q = send(by_owner(estimated_returns), ACT)

    moves = by_owner(chosen_move_ids).reshape(across, along, cores, rows, own)
    give = lax.dynamic_index_in_dim(moves, 1 - at[2], 2, keepdims=False)
    from_core = shifted_by(give, "core", 1)
    chunks = call(split_body, [shape((cores, across, rows, own), i32)] * along, 1, 2)(at, moves, from_core)
    arrived = [chunks[0]]
    for k in range(1, along):
        arrived.append(shifted_by(chunks[k], "z", k))

    row_shape = shape((1, LANES), f32)

    def sums_of_chips(part):
        chip = part + shifted_by(part, "core", 1)
        return send(jnp.broadcast_to(chip[None], (everyone // cores, 1, LANES)), CHIPS)

    top, eta, eps, part = call(
        functools.partial(first_body, samples), [shape((1, own), f32), row_shape, row_shape, row_shape], 2, 1
    )(previous_eta, trust_region_epsilon, q)
    for i in range(ITERS - 1):
        gathered = sums_of_chips(part)
        eta, part = call(
            functools.partial(step_body, samples, states), [row_shape, row_shape], 0, 5
        )(eps, q, top, eta, gathered)
        if i == 1:
            chunks = call(merge_body, [shape((along, cores, rows, own), i32)] * across, 1, 1 + along)(at, eta, *arrived)
            ids = [chunks[0]]
            for j in range(1, across):
                ids.append(shifted_by(chunks[j], "x", j))
    gathered = sums_of_chips(part)
    eta, back = call(
        functools.partial(last_body, samples, states),
        [row_shape, shape((peers // cores, 1, 2 * own), f32)], 0, 5,
    )(eps, q, top, eta, gathered)
    from_same = send(back, PLANE)
    from_other = shifted_by(from_same, "core", 1)
    goal = call(
        functools.partial(goal_body, samples), shape((NACT, own), f32), 1, 3 + across, flops=20_000_000
    )(at, q, back, eta, *ids)

    steps = 4
    weights = pl.pallas_call(
        functools.partial(weights_body, steps),
        out_shape=shape((rows, width), f32),
        in_specs=[SMEM] + [VMEM] * 4,
        out_specs=pl.BlockSpec(memory_space=pl.ANY),
        scratch_shapes=[pltpu.VMEM((rows, width), f32), pltpu.SemaphoreType.DMA((steps,))],
        compiler_params=PARAMS,
        cost_estimate=pl.CostEstimate(flops=1_000_000, bytes_accessed=2_000_000, transcendentals=262_144),
        name="weights",
    )(at, eta, estimated_returns, from_same, from_other)
    return weights, goal, eta[0, :1]


def solution(mesh):
    split = Mesh(mesh.devices.reshape(4, 8, 2, mesh.shape["rep"]), (*ACT, "rep"))
    placed = (P(ACT, "rep"), P(ACT, "rep"), P(), P())
    return jax.shard_map(
        on_device,
        mesh=split,
        in_specs=placed,
        out_specs=(P(ACT, "rep"), P(None, ALL), P()),
        check_vma=False,
    )
```

```python
import functools
import jax
import jax.numpy as jnp
from jax import lax
from jax.experimental import pallas as pl
from jax.experimental.pallas import tpu as pltpu
from jax.sharding import Mesh
from jax.sharding import PartitionSpec as P

NACT = 18
ITERS = 3
LANES = 128
LOG2E = 1.4426950408889634
ACT = ("x", "z", "core")
ALL = ("rep", "x", "z", "core")
CHIPS = ("rep", "x", "z")
PLANE = ("x", "z")
VMEM = pl.BlockSpec(memory_space=pltpu.VMEM)
SMEM = pl.BlockSpec(memory_space=pltpu.SMEM)
PARAMS = pltpu.CompilerParams(vmem_limit_bytes=8 * 1024 * 1024)


def call(body, out_shape, n_smem, n_vmem, flops=1_000_000):
    n_out = len(out_shape) if isinstance(out_shape, (tuple, list)) else None
    return pl.pallas_call(
        body,
        out_shape=out_shape,
        in_specs=[SMEM] * n_smem + [VMEM] * n_vmem,
        out_specs=VMEM if n_out is None else [VMEM] * n_out,
        compiler_params=PARAMS,
        cost_estimate=pl.CostEstimate(flops=flops, bytes_accessed=2_000_000, transcendentals=262_144),
    )


def partial_sums(q_ref, top, eta, samples):
    blocks, rows, states = q_ref.shape
    inverse = jnp.broadcast_to((1.0 / eta)[:, :1], (rows, states))
    rate = inverse * LOG2E
    top_rows = jnp.broadcast_to(top, (rows, states))

    def step(i, sums):
        z, c1, c2 = sums
        shifted = q_ref[i] - top_rows
        expo = jnp.exp2(shifted * rate)
        first = expo * shifted
        return z + expo, c1 + first, c2 + first * shifted

    zero = jnp.zeros((rows, states), jnp.float32)
    z, c1, c2 = lax.fori_loop(0, blocks, step, (zero, zero, zero), unroll=8)
    z, c1, c2 = (jnp.sum(v, axis=0, keepdims=True) for v in (z, c1, c2))
    mean = c1 / z
    kl = mean * inverse[:1] - jnp.log(z) + jnp.log(jnp.float32(samples))
    spread = c2 / z - mean * mean
    lane = lax.broadcasted_iota(jnp.int32, (1, LANES), 1)
    kl_sum = jnp.sum(kl, axis=1, keepdims=True)
    spread_sum = jnp.sum(spread, axis=1, keepdims=True)
    return jnp.where(lane == 0, kl_sum, jnp.where(lane == 1, spread_sum, 0.0))


def next_eta(gathered_ref, eta, eps, states):
    total = jnp.sum(gathered_ref[...], axis=0, keepdims=True) * jnp.float32(1.0 / states)
    divergence = jnp.broadcast_to(total[:, 0:1], eta.shape)
    deviation = jnp.broadcast_to(total[:, 1:2], eta.shape)
    change = (eps - divergence) * eta / (1.0 + deviation / eta)
    return eta * jnp.exp(-jnp.tanh(change))


def row(scalar):
    return jnp.full((1, LANES), scalar, jnp.float32)


def first_body(samples, eta_ref, eps_ref, q_ref, top_ref, eta_out, eps_out, part_ref):
    top8 = q_ref[0]
    top8 = lax.fori_loop(1, q_ref.shape[0], lambda i, m: jnp.maximum(m, q_ref[i]), top8)
    top = jnp.max(top8, axis=0, keepdims=True)
    top_ref[...] = top
    eta = row(eta_ref[0])
    eta_out[...] = eta
    eps_out[...] = row(eps_ref[0])
    part_ref[...] = partial_sums(q_ref, top, eta, samples)


def step_body(samples, states, eps_ref, q_ref, top_ref, eta_ref, gathered_ref, eta_out, part_ref):
    eta = next_eta(gathered_ref, eta_ref[...], eps_ref[...], states)
    eta_out[...] = eta
    part_ref[...] = partial_sums(q_ref, top_ref[...], eta, samples)


def last_body(samples, states, eps_ref, q_ref, top_ref, eta_ref, gathered_ref, eta_out, final_ref, back_ref):
    eta = next_eta(gathered_ref, eta_ref[...], eps_ref[...], states)
    eta_out[...] = eta
    blocks, rows, width = q_ref.shape
    rate = jnp.broadcast_to((LOG2E / eta)[:, :1], (rows, width))
    top = top_ref[...]
    top_rows = jnp.broadcast_to(top, (rows, width))
    z = lax.fori_loop(
        0, blocks, lambda i, z: z + jnp.exp2((q_ref[i] - top_rows) * rate),
        jnp.zeros((rows, width), jnp.float32), unroll=8)
    scale = jnp.float32(samples) / jnp.sum(z, axis=0, keepdims=True)
    tiles = [v[:, t : t + LANES] for v in (top, scale) for t in range(0, width, LANES)]
    tiles = jnp.concatenate(tiles, axis=0)
    back_ref[...] = jnp.broadcast_to(tiles[None], back_ref.shape)
    final_ref[0] = tiles
    final_ref[1] = jnp.broadcast_to(eta, tiles.shape)


def split_body(at_ref, ids_ref, from_core_ref, *out_refs):
    z, core = at_ref[1], at_ref[2]
    hops = len(out_refs)
    for k, out_ref in enumerate(out_refs):
        to = lax.rem(z + k, hops)
        for x in range(out_ref.shape[1]):
            out_ref[0, x] = ids_ref[x, to, core]
            out_ref[1, x] = from_core_ref[x, to]


def merge_body(at_ref, _, *refs):
    hops = len(refs) * 2 // 3
    in_refs, out_refs = refs[:hops], refs[hops:]
    for j, out_ref in enumerate(out_refs):
        to = lax.rem(at_ref[0] + j, len(out_refs))
        for k, in_ref in enumerate(in_refs):
            out_ref[k] = in_ref[:, to]


def goal_body(samples, at_ref, q_ref, final_ref, *refs):
    ids_refs, goal_ref = refs[:-1], refs[-1]
    across, along, cores = len(ids_refs), ids_refs[0].shape[0], ids_refs[0].shape[1]
    _, rows, width = q_ref.shape
    rate = LOG2E / final_ref[1]
    x, z, core = at_ref[0], at_ref[1], at_ref[2]
    for tile in range(width // LANES):
        at = slice(tile * LANES, (tile + 1) * LANES)
        top_rows = jnp.broadcast_to(final_ref[0, tile : tile + 1], (rows, LANES))
        tiles = width // LANES
        scale = final_ref[0, tiles + tile : tiles + tile + 1] * jnp.float32(1.0 / samples)
        sums = (jnp.zeros((rows, LANES), jnp.float32),) * NACT
        for j, ids_ref in enumerate(ids_refs):
            from_x = lax.rem(x + across - j , across)

            def step(k, sums):
                from_z = lax.rem(z + along - k , along)
                for c in range(cores):
                    from_core = core if c == 0 else 1 - core
                    holder = (from_x * along + from_z) * cores + from_core
                    expo = jnp.exp2((q_ref[holder, :, at] - top_rows) * rate)
                    ids = ids_ref[k, c, :, at]
                    sums = tuple(s + jnp.where(ids == n, expo, 0.0) for n, s in enumerate(sums))
                return sums

            sums = lax.fori_loop(0, along, step, sums, unroll=2)
        for n, s in enumerate(sums):
            goal_ref[n : n + 1, at] = jnp.sum(s, axis=0, keepdims=True) * scale


def weights_body(steps, at_ref, final_ref, x_ref, same_ref, other_ref, out_ref, held, sems):
    rows, width = x_ref.shape
    chips, both, _ = same_ref.shape
    tiles = both // 2
    rate = LOG2E / final_ref[1]
    core = at_ref[2]
    copies = []
    for step in range(steps):
        for chip in range(step * chips // steps, (step + 1) * chips // steps):
            for from_ref, owner in ((same_ref, chip * 2 + core), (other_ref, chip * 2 + 1 - core)):
                for t in range(tiles):
                    at = pl.ds(pl.multiple_of((owner * tiles + t) * LANES, LANES), LANES)
                    top = jnp.broadcast_to(from_ref[chip, t : t + 1], (rows, LANES))
                    scale = jnp.broadcast_to(from_ref[chip, tiles + t : tiles + t + 1], (rows, LANES))
                    held[:, at] = jnp.exp2((x_ref[:, at] - top) * rate) * scale
        part = pl.ds(step * width // steps, width // steps)
        copies.append(pltpu.make_async_copy(held.at[:, part], out_ref.at[:, part], sems.at[step]))
        copies[-1].start()
    for copy in copies:
        copy.wait()


def turned(axes):
    order = [0]
    for size in (lax.axis_size(a) for a in axes):
        turn = (2 if len(order) == 1 else 1) if axes[0] == "rep" else 0
        order = [n * size + (i + turn) % size for n in order for i in range(size)]
    return order


def send(blocks, axes):
    return lax.all_to_all(
        blocks, axes, split_axis=0, concat_axis=0, tiled=True, axis_index_groups=[turned(axes)]
    )


def shifted_by(v, axis, hops):
    size = lax.axis_size(axis)
    return lax.ppermute(v, axis, [(i, (i + hops) % size) for i in range(size)])


def on_device(estimated_returns, chosen_move_ids, previous_eta, trust_region_epsilon):
    across, along, cores = (lax.axis_size(a) for a in ACT)
    peers = lax.axis_size(ACT)
    everyone = peers * lax.axis_size("rep")
    rows, width = estimated_returns.shape
    own = width // peers
    samples, states = rows * peers, width * lax.axis_size("rep")
    f32, i32 = jnp.float32, jnp.int32
    shape = jax.ShapeDtypeStruct
    at = jnp.stack([lax.axis_index(a) for a in ACT])

    def by_owner(v):
        return v.reshape(rows, peers, own).transpose(1, 0, 2)

    q = send(by_owner(estimated_returns), ACT)

    moves = by_owner(chosen_move_ids).reshape(across, along, cores, rows, own)
    give = lax.dynamic_index_in_dim(moves, 1 - at[2], 2, keepdims=False)
    from_core = shifted_by(give, "core", 1)
    chunks = call(split_body, [shape((cores, across, rows, own), i32)] * along, 1, 2)(at, moves, from_core)
    arrived = [chunks[0]]
    for k in range(1, along):
        arrived.append(shifted_by(chunks[k], "z", k))

    row_shape = shape((1, LANES), f32)

    def sums_of_chips(part):
        chip = part + shifted_by(part, "core", 1)
        copies = jnp.broadcast_to(chip[None], (everyone // cores, 1, LANES))
        return send(copies, CHIPS).reshape(everyone // cores, LANES)

    top, eta, eps, part = call(
        functools.partial(first_body, samples), [shape((1, own), f32), row_shape, row_shape, row_shape], 2, 1
    )(previous_eta, trust_region_epsilon, q)
    for i in range(ITERS - 1):
        gathered = sums_of_chips(part)
        eta, part = call(
            functools.partial(step_body, samples, states), [row_shape, row_shape], 0, 5
        )(eps, q, top, eta, gathered)
        if i == 1:
            chunks = call(merge_body, [shape((along, cores, rows, own), i32)] * across, 1, 1 + along)(at, eta, *arrived)
            ids = [chunks[0]]
            for j in range(1, across):
                ids.append(shifted_by(chunks[j], "x", j))
    gathered = sums_of_chips(part)
    eta, final, back = call(
        functools.partial(last_body, samples, states),
        [row_shape, shape((2, 2 * own // LANES, LANES), f32), shape((peers // cores, 2 * own // LANES, LANES), f32)], 0, 5,
    )(eps, q, top, eta, gathered)
    from_same = send(back, PLANE)
    from_other = shifted_by(from_same, "core", 1)
    goal = call(
        functools.partial(goal_body, samples), shape((NACT, own), f32), 1, 2 + across, flops=20_000_000
    )(at, q, final, *ids)

    steps = 4
    weights_kernel = pl.pallas_call(
        functools.partial(weights_body, steps),
        out_shape=shape((rows, width), f32),
        in_specs=[SMEM] + [VMEM] * 4,
        out_specs=pl.BlockSpec(memory_space=pl.ANY),
        scratch_shapes=[pltpu.VMEM((rows, width), f32), pltpu.SemaphoreType.DMA((steps,))],
        compiler_params=PARAMS,
        cost_estimate=pl.CostEstimate(flops=1_000_000, bytes_accessed=2_000_000, transcendentals=262_144),
        name="weights",
    )
    weights = weights_kernel(at, final, estimated_returns, from_same, from_other)
    return weights, goal, eta[0, :1]


def solution(mesh):
    split = Mesh(mesh.devices.reshape(4, 8, 2, mesh.shape["rep"]), (*ACT, "rep"))
    placed = (P(ACT, "rep"), P(ACT, "rep"), P(), P())
    return jax.shard_map(
        on_device,
        mesh=split,
        in_specs=placed,
        out_specs=(P(ACT, "rep"), P(None, ALL), P()),
        check_vma=False,
    )
```

```python
import functools
import jax
import jax.numpy as jnp
from jax import lax
from jax.experimental import pallas as pl
from jax.experimental.pallas import tpu as pltpu
from jax.sharding import Mesh
from jax.sharding import PartitionSpec as P

NACT = 18
ITERS = 3
LANES = 128
LOG2E = 1.4426950408889634
ACT = ("x", "z", "core")
ALL = ("rep", "x", "z", "core")
CHIPS = ("rep", "x", "z")
PLANE = ("x", "z")
VMEM = pl.BlockSpec(memory_space=pltpu.VMEM)
SMEM = pl.BlockSpec(memory_space=pltpu.SMEM)
PARAMS = pltpu.CompilerParams(vmem_limit_bytes=8 * 1024 * 1024)


def call(body, out_shape, n_smem, n_vmem, flops=1_000_000):
    n_out = len(out_shape) if isinstance(out_shape, (tuple, list)) else None
    return pl.pallas_call(
        body,
        out_shape=out_shape,
        in_specs=[SMEM] * n_smem + [VMEM] * n_vmem,
        out_specs=VMEM if n_out is None else [VMEM] * n_out,
        compiler_params=PARAMS,
        cost_estimate=pl.CostEstimate(flops=flops, bytes_accessed=2_000_000, transcendentals=262_144),
    )


def partial_sums(q_ref, top, eta, samples):
    blocks, rows, states = q_ref.shape
    inverse = jnp.broadcast_to((1.0 / eta)[:, :1], (rows, states))
    rate = inverse * LOG2E
    top_rows = jnp.broadcast_to(top, (rows, states))

    def step(i, sums):
        z, c1, c2 = sums
        shifted = q_ref[i] - top_rows
        expo = jnp.exp2(shifted * rate)
        first = expo * shifted
        return z + expo, c1 + first, c2 + first * shifted

    zero = jnp.zeros((rows, states), jnp.float32)
    z, c1, c2 = lax.fori_loop(0, blocks, step, (zero, zero, zero), unroll=16)
    z, c1, c2 = (jnp.sum(v, axis=0, keepdims=True) for v in (z, c1, c2))
    mean = c1 / z
    kl = mean * inverse[:1] - jnp.log(z) + jnp.log(jnp.float32(samples))
    spread = c2 / z - mean * mean
    lane = lax.broadcasted_iota(jnp.int32, (1, LANES), 1)
    kl_sum = jnp.sum(kl, axis=1, keepdims=True)
    spread_sum = jnp.sum(spread, axis=1, keepdims=True)
    return jnp.where(lane == 0, kl_sum, jnp.where(lane == 1, spread_sum, 0.0))


def next_eta(gathered_ref, eta, eps, states):
    total = jnp.sum(gathered_ref[...], axis=0, keepdims=True) * jnp.float32(1.0 / states)
    divergence = jnp.broadcast_to(total[:, 0:1], eta.shape)
    deviation = jnp.broadcast_to(total[:, 1:2], eta.shape)
    change = (eps - divergence) * eta / (1.0 + deviation / eta)
    return eta * jnp.exp(-jnp.tanh(change))


def row(scalar):
    return jnp.full((1, LANES), scalar, jnp.float32)


def first_body(samples, eta_ref, eps_ref, q_ref, top_ref, eta_out, eps_out, part_ref):
    top8 = q_ref[0]
    top8 = lax.fori_loop(1, q_ref.shape[0], lambda i, m: jnp.maximum(m, q_ref[i]), top8, unroll=9)
    top = jnp.max(top8, axis=0, keepdims=True)
    top_ref[...] = top
    eta = row(eta_ref[0])
    eta_out[...] = eta
    eps_out[...] = row(eps_ref[0])
    part_ref[...] = partial_sums(q_ref, top, eta, samples)


def step_body(samples, states, eps_ref, q_ref, top_ref, eta_ref, gathered_ref, eta_out, part_ref):
    eta = next_eta(gathered_ref, eta_ref[...], eps_ref[...], states)
    eta_out[...] = eta
    part_ref[...] = partial_sums(q_ref, top_ref[...], eta, samples)


def last_body(samples, states, eps_ref, q_ref, top_ref, eta_ref, gathered_ref, eta_out, final_ref, back_ref):
    eta = next_eta(gathered_ref, eta_ref[...], eps_ref[...], states)
    eta_out[...] = eta
    blocks, rows, width = q_ref.shape
    rate = jnp.broadcast_to((LOG2E / eta)[:, :1], (rows, width))
    top = top_ref[...]
    top_rows = jnp.broadcast_to(top, (rows, width))
    z = lax.fori_loop(
        0, blocks, lambda i, z: z + jnp.exp2((q_ref[i] - top_rows) * rate),
        jnp.zeros((rows, width), jnp.float32), unroll=16)
    scale = jnp.float32(samples) / jnp.sum(z, axis=0, keepdims=True)
    tiles = [v[:, t : t + LANES] for v in (top, scale) for t in range(0, width, LANES)]
    tiles = jnp.concatenate(tiles, axis=0)
    back_ref[...] = jnp.broadcast_to(tiles[None], back_ref.shape)
    final_ref[0] = tiles
    final_ref[1] = jnp.broadcast_to(eta, tiles.shape)


def split_body(at_ref, ids_ref, from_core_ref, *out_refs):
    z, core = at_ref[1], at_ref[2]
    hops = len(out_refs)
    for k, out_ref in enumerate(out_refs):
        to = lax.rem(z + k, hops)
        for x in range(out_ref.shape[1]):
            out_ref[0, x] = ids_ref[x, to, core]
            out_ref[1, x] = from_core_ref[x, to]


def merge_body(at_ref, _, *refs):
    hops = len(refs) * 2 // 3
    in_refs, out_refs = refs[:hops], refs[hops:]
    for j, out_ref in enumerate(out_refs):
        to = lax.rem(at_ref[0] + j, len(out_refs))
        for k, in_ref in enumerate(in_refs):
            out_ref[k] = in_ref[:, to]


def goal_body(samples, at_ref, q_ref, final_ref, *refs):
    ids_refs, goal_ref = refs[:-1], refs[-1]
    across, along, cores = len(ids_refs), ids_refs[0].shape[0], ids_refs[0].shape[1]
    _, rows, width = q_ref.shape
    rate = LOG2E / final_ref[1]
    x, z, core = at_ref[0], at_ref[1], at_ref[2]
    for tile in range(width // LANES):
        at = slice(tile * LANES, (tile + 1) * LANES)
        top_rows = jnp.broadcast_to(final_ref[0, tile : tile + 1], (rows, LANES))
        tiles = width // LANES
        scale = final_ref[0, tiles + tile : tiles + tile + 1] * jnp.float32(1.0 / samples)
        sums = (jnp.zeros((rows, LANES), jnp.float32),) * NACT
        for j, ids_ref in enumerate(ids_refs):
            from_x = lax.rem(x + across - j , across)

            def step(k, sums):
                from_z = lax.rem(z + along - k , along)
                for c in range(cores):
                    from_core = core if c == 0 else 1 - core
                    holder = (from_x * along + from_z) * cores + from_core
                    expo = jnp.exp2((q_ref[holder, :, at] - top_rows) * rate)
                    ids = ids_ref[k, c, :, at]
                    sums = tuple(s + jnp.where(ids == n, expo, 0.0) for n, s in enumerate(sums))
                return sums

            sums = lax.fori_loop(0, along, step, sums, unroll=2)
        for n, s in enumerate(sums):
            goal_ref[n : n + 1, at] = jnp.sum(s, axis=0, keepdims=True) * scale


def weights_body(steps, at_ref, final_ref, x_ref, same_ref, other_ref, out_ref, held, sems):
    rows, width = x_ref.shape
    chips, both, _ = same_ref.shape
    tiles = both // 2
    rate = LOG2E / final_ref[1]
    core = at_ref[2]
    copies = []
    for step in range(steps):
        for chip in range(step * chips // steps, (step + 1) * chips // steps):
            for from_ref, owner in ((same_ref, chip * 2 + core), (other_ref, chip * 2 + 1 - core)):
                for t in range(tiles):
                    at = pl.ds(pl.multiple_of((owner * tiles + t) * LANES, LANES), LANES)
                    top = jnp.broadcast_to(from_ref[chip, t : t + 1], (rows, LANES))
                    scale = jnp.broadcast_to(from_ref[chip, tiles + t : tiles + t + 1], (rows, LANES))
                    held[:, at] = jnp.exp2((x_ref[:, at] - top) * rate) * scale
        part = pl.ds(step * width // steps, width // steps)
        copies.append(pltpu.make_async_copy(held.at[:, part], out_ref.at[:, part], sems.at[step]))
        copies[-1].start()
    for copy in copies:
        copy.wait()


def turned(axes):
    order = [0]
    for size in (lax.axis_size(a) for a in axes):
        turn = (2 if len(order) == 1 else 1) if axes[0] == "rep" else 0
        order = [n * size + (i + turn) % size for n in order for i in range(size)]
    return order


def send(blocks, axes):
    return lax.all_to_all(
        blocks, axes, split_axis=0, concat_axis=0, tiled=True, axis_index_groups=[turned(axes)]
    )


def shifted_by(v, axis, hops):
    size = lax.axis_size(axis)
    return lax.ppermute(v, axis, [(i, (i + hops) % size) for i in range(size)])


def on_device(estimated_returns, chosen_move_ids, previous_eta, trust_region_epsilon):
    across, along, cores = (lax.axis_size(a) for a in ACT)
    peers = lax.axis_size(ACT)
    everyone = peers * lax.axis_size("rep")
    rows, width = estimated_returns.shape
    own = width // peers
    samples, states = rows * peers, width * lax.axis_size("rep")
    f32, i32 = jnp.float32, jnp.int32
    shape = jax.ShapeDtypeStruct
    at = jnp.stack([lax.axis_index(a) for a in ACT])

    def by_owner(v):
        return v.reshape(rows, peers, own).transpose(1, 0, 2)

    q = send(by_owner(estimated_returns), ACT)

    moves = by_owner(chosen_move_ids).reshape(across, along, cores, rows, own)
    give = lax.dynamic_index_in_dim(moves, 1 - at[2], 2, keepdims=False)
    from_core = shifted_by(give, "core", 1)
    chunks = call(split_body, [shape((cores, across, rows, own), i32)] * along, 1, 2)(at, moves, from_core)
    arrived = [chunks[0]]
    for k in range(1, along):
        arrived.append(shifted_by(chunks[k], "z", k))

    row_shape = shape((1, LANES), f32)

    def sums_of_chips(part):
        chip = part + shifted_by(part, "core", 1)
        copies = jnp.broadcast_to(chip[None], (everyone // cores, 1, LANES))
        return send(copies, CHIPS).reshape(everyone // cores, LANES)

    top, eta, eps, part = call(
        functools.partial(first_body, samples), [shape((1, own), f32), row_shape, row_shape, row_shape], 2, 1
    )(previous_eta, trust_region_epsilon, q)
    for i in range(ITERS - 1):
        gathered = sums_of_chips(part)
        eta, part = call(
            functools.partial(step_body, samples, states), [row_shape, row_shape], 0, 5
        )(eps, q, top, eta, gathered)
        if i == 1:
            chunks = call(merge_body, [shape((along, cores, rows, own), i32)] * across, 1, 1 + along)(at, eta, *arrived)
            ids = [chunks[0]]
            for j in range(1, across):
                ids.append(shifted_by(chunks[j], "x", j))
    gathered = sums_of_chips(part)
    eta, final, back = call(
        functools.partial(last_body, samples, states),
        [row_shape, shape((2, 2 * own // LANES, LANES), f32), shape((peers // cores, 2 * own // LANES, LANES), f32)], 0, 5,
    )(eps, q, top, eta, gathered)
    from_same = send(back, PLANE)
    from_other = shifted_by(from_same, "core", 1)
    goal = call(
        functools.partial(goal_body, samples), shape((NACT, own), f32), 1, 2 + across, flops=20_000_000
    )(at, q, final, *ids)

    steps = 4
    weights_kernel = pl.pallas_call(
        functools.partial(weights_body, steps),
        out_shape=shape((rows, width), f32),
        in_specs=[SMEM] + [VMEM] * 4,
        out_specs=pl.BlockSpec(memory_space=pl.ANY),
        scratch_shapes=[pltpu.VMEM((rows, width), f32), pltpu.SemaphoreType.DMA((steps,))],
        compiler_params=PARAMS,
        cost_estimate=pl.CostEstimate(flops=1_000_000, bytes_accessed=2_000_000, transcendentals=262_144),
        name="weights",
    )
    weights = weights_kernel(at, final, estimated_returns, from_same, from_other)
    return weights, goal, eta[0, :1]


def solution(mesh):
    split = Mesh(mesh.devices.reshape(4, 8, 2, mesh.shape["rep"]), (*ACT, "rep"))
    placed = (P(ACT, "rep"), P(ACT, "rep"), P(), P())
    return jax.shard_map(
        on_device,
        mesh=split,
        in_specs=placed,
        out_specs=(P(ACT, "rep"), P(None, ALL), P()),
        check_vma=False,
    )
```
